256 devices in a mesh: section: 8 (over y, core), replica: 32 (over z, x).
Axes of the slice: x: 4, y: 4, z: 8, core: 2. Of those that a mesh axis runs over, the one named last changes fastest.
Arguments:
- gradient: bfloat16 [1024, 131072], P('section', 'replica'), may hold values from -1300 to 1300
- residual: float32 [1024, 131072], P('section', 'replica'), may hold values from -6 to 6
- block_ids: int32 [8, 256], P('section', 'replica'), may hold values from 0 to 15, as said below
- block_counts: int32 [8, 32], P('section', 'replica'), may hold values from 1 to 8, as said below
Outputs:
- new_residual: float32 [1024, 131072], P('section', 'replica')
- update: bfloat16 [1024, 4096], P('section', 'replica')
The draws below stay inside these ranges and needn't reach their ends.
Inputs may be any that keep to these rules, and one draw needn't show every extreme that they name: `block_ids`: each device's 8 block numbers are distinct; only the first block_counts of them are selected. `block_counts`: in every section some replica selects exactly 8 blocks; the others select at most 4.
All inputs are finite; a program needn't handle non-finite values.
Results may differ from the reference program's by a relative error of at most 0.013.
Values may be sent and summed in bfloat16 or wider, within the bound.
No kernel may reach another device: no remote copies, remote signals or barrier semaphores. Data moves between devices by JAX's collectives and lax.ppermute only.
A program may use at most 64 MiB of HBM per device.

```python
import math
import jax
import jax.numpy as jnp
from jax import lax

D = 4096
ROWS = 128
BLK = 8
KMAX = 8
SECTIONS = 8
REPLICAS = 32


def draw_gradient(key, part):
    key_rows, key_base, key_common, key_level, key_mix, key_slice, key_column = jax.random.split(key, 7)
    slice_width = D // REPLICAS
    row_scale = jnp.exp(jax.random.uniform(key_rows, (SECTIONS * ROWS, REPLICAS, 1), jnp.float32, 0.0, math.log(10.0)))
    section_of_row = (jnp.arange(SECTIONS * ROWS, dtype=jnp.int32) // ROWS).astype(jnp.int32)
    section_scale = 1.0 + 2.0 * section_of_row.astype(jnp.float32) / max(SECTIONS - 1, 1)
    slice_of_column = (jnp.arange(D, dtype=jnp.int32) // slice_width).astype(jnp.int32)
    slice_scale = jnp.exp(jax.random.uniform(key_slice, (REPLICAS,), jnp.float32, 0.0, math.log(4.0)))
    column_rough = jax.random.uniform(key_column, (D,), jnp.float32, 0.6, 1.4)
    column_scale = slice_scale[slice_of_column] * column_rough
    section_level = jax.random.uniform(key_level, (SECTIONS,), jnp.float32, 0.0, 1.2)
    slice_mix = jax.random.uniform(key_mix, (SECTIONS, REPLICAS), jnp.float32, 0.0, 1.0)
    mix_weight = section_level[:, None] * slice_mix
    weight_grid = mix_weight[section_of_row][:, slice_of_column]
    base_draw = jnp.clip(jax.random.normal(key_base, (SECTIONS * ROWS, REPLICAS, D), jnp.float32), -4.0, 4.0)
    common_part = jnp.clip(jax.random.normal(key_common, (SECTIONS * ROWS, 1, D), jnp.float32), -3.0, 3.0)
    base_draw = base_draw + weight_grid[:, None, :] * common_part
    values = base_draw * row_scale * section_scale[:, None, None] * column_scale[None, None, :]
    return values.reshape(SECTIONS * ROWS, REPLICAS * D).astype(jnp.bfloat16)


def draw_block_ids(key, part):
    block_total = ROWS // BLK
    scores = jax.random.randint(key, (SECTIONS, REPLICAS, block_total), 0, 1 << 20) * block_total + jnp.arange(block_total, dtype=jnp.int32)
    ordering = jnp.argsort(scores, axis=-1, stable=True)
    return ordering[..., :KMAX].reshape(SECTIONS, REPLICAS * KMAX).astype(jnp.int32)


def draw_block_counts(key, part):
    key_base, key_busy = jax.random.split(key)
    base_draw = jax.random.randint(key_base, (SECTIONS, REPLICAS), 1, KMAX // 2 + 1)
    busy_replica = jax.random.randint(key_busy, (SECTIONS, 1), 0, REPLICAS)
    placed = jnp.arange(REPLICAS, dtype=jnp.int32)[None, :] == busy_replica
    return jnp.where(placed, KMAX, base_draw).astype(jnp.int32)


def block_scale(stream_key, extent, cuts, low, top_value):
    level, own = 1.0, jax.random.fold_in(stream_key, 6)
    for axis_at, shards_of in cuts:
        draws = jnp.exp(jax.random.uniform(jax.random.fold_in(own, axis_at), (shards_of,), jnp.float32, low / len(cuts), top_value / len(cuts)))
        level = level * jnp.repeat(draws, extent[axis_at] // shards_of).reshape([-1 if axis == axis_at else 1 for axis in range(len(extent))])
    return level


def centred(rng, dims, scale, reach, shards=(), kind=jnp.bfloat16):
    array = scale * jax.random.normal(rng, dims, jnp.float32)
    if shards:
        array = array * block_scale(rng, dims, shards, -0.22, 0.18)
    return jnp.clip(array, -reach, reach).astype(kind)


def setup_inputs(seed: int = 0) -> dict:
    streams_of = jax.random.split(jax.random.key(seed), 5)
    gradient = draw_gradient(jax.random.fold_in(streams_of[4], 71), 0)
    residual = centred(streams_of[1], (SECTIONS * ROWS, REPLICAS * D), 1.0, 6.0, ((0, 8), (1, 32)), jnp.float32)
    block_ids = draw_block_ids(jax.random.fold_in(streams_of[4], 71), 0)
    block_counts = draw_block_counts(jax.random.fold_in(streams_of[4], 71), 0)
    return dict(gradient=gradient, residual=residual, block_ids=block_ids, block_counts=block_counts)


scale_level = 1.0
epsilon = 1e-06

def reference(gradient, residual, block_ids, block_counts):
    block_total = ROWS // BLK
    accumulated = gradient.astype(jnp.float32) + residual
    slot_ids = block_ids.reshape(SECTIONS, REPLICAS, KMAX)
    live_slot = jnp.arange(KMAX, dtype=jnp.int32)[None, None, :] < block_counts[:, :, None]
    hit_table = (slot_ids[..., None] == jnp.arange(block_total, dtype=jnp.int32)) & live_slot[..., None]
    chosen = jnp.any(hit_table, axis=2)
    block_mask = jnp.transpose(chosen, (0, 2, 1))[:, :, None, :, None]
    shaped = accumulated.reshape(SECTIONS, block_total, BLK, REPLICAS, D)
    sent = jnp.where(block_mask, shaped.astype(jnp.bfloat16).astype(jnp.float32), jnp.float32(0.0))
    new_residual = (shaped - sent).reshape(accumulated.shape)
    summed = lax.optimization_barrier(jnp.sum(sent, axis=3)).reshape(SECTIONS * ROWS, D)
    norm_total = jnp.sum(summed * summed)
    root_mean = jnp.sqrt(norm_total / (SECTIONS * ROWS * D) + epsilon)
    clip_factor = scale_level / root_mean
    update = (summed * clip_factor).astype(jnp.bfloat16)
    return (new_residual, update)
```

```python
import jax
import jax.numpy as jnp
from jax import lax
from jax.experimental import pallas as pl
from jax.experimental.pallas import tpu as pltpu
from jax.sharding import Mesh
from jax.sharding import PartitionSpec as P

BLK = 8
LANES = 128
REPLICA = ("replica_0", "replica_1")
SECTION = ("section_0", "section_1")
CHIPS = ("section_0", "replica_0", "replica_1")

scale_level = 1.0
epsilon = 1e-06


def pack_kernel(ids, counts, gradient, residual, packed, grad_buf, res_buf, grad_sem, res_sem):
    slots = grad_buf.shape[0]
    dests = packed.shape[0]
    copies = []
    for j in range(slots):
        rows = pl.ds(pl.multiple_of(ids[0, j] * BLK, BLK), BLK)
        copies.append(
            (
                pltpu.make_async_copy(gradient.at[rows, :], grad_buf.at[j], grad_sem.at[j]),
                pltpu.make_async_copy(residual.at[rows, :], res_buf.at[j], res_sem.at[j]),
            )
        )
    for pair in copies:
        for copy in pair:
            copy.start()
    lane = lax.broadcasted_iota(jnp.int32, (BLK, LANES), 1)
    slot_of = (lane // BLK) % slots
    code = jnp.full((BLK, LANES), -1, jnp.int32)
    for j in range(slots):
        row = jnp.where(j < counts[0, 0], ids[0, j] * BLK, -2 * LANES)
        code = jnp.where(slot_of == j, row + lane % BLK, code)
    code = jnp.maximum(code, -1).astype(jnp.float32).astype(jnp.bfloat16)
    for d in range(dests):
        packed[d, slots * BLK :, :] = code
    for j, pair in enumerate(copies):
        for copy in pair:
            copy.wait()
        for d in range(dests):
            cols = slice(d * LANES, (d + 1) * LANES)
            total = grad_buf[j, :, cols].astype(jnp.float32) + res_buf[j, :, cols]
            packed[d, j * BLK : (j + 1) * BLK, :] = total.astype(jnp.bfloat16)


def pack(gradient, residual, block_ids, block_counts, replicas):
    width = gradient.shape[1]
    slots = block_ids.shape[1]
    return pl.pallas_call(
        pack_kernel,
        out_shape=jax.ShapeDtypeStruct((replicas, (slots + 1) * BLK, width // replicas), jnp.bfloat16),
        in_specs=[
            pl.BlockSpec(memory_space=pltpu.SMEM),
            pl.BlockSpec(memory_space=pltpu.SMEM),
            pl.BlockSpec(memory_space=pl.ANY),
            pl.BlockSpec(memory_space=pl.ANY),
        ],
        out_specs=pl.BlockSpec(memory_space=pltpu.VMEM),
        scratch_shapes=[
            pltpu.VMEM((slots, BLK, width), gradient.dtype),
            pltpu.VMEM((slots, BLK, width), residual.dtype),
            pltpu.SemaphoreType.DMA((slots,)),
            pltpu.SemaphoreType.DMA((slots,)),
        ],
        name="pack",
    )(block_ids, block_counts, gradient, residual)


def deposit_kernel(received, summed, squares):
    sources, rows, lanes = received.shape
    live = rows - BLK
    total_rows = summed.shape[0]
    low_half = lax.broadcasted_iota(jnp.int32, (BLK, lanes), 1) < live
    sub = lax.broadcasted_iota(jnp.int32, (BLK, lanes), 0)
    row_ids = [(sub + g * BLK).astype(jnp.float32) for g in range(total_rows // BLK)]
    total = jnp.zeros((total_rows, lanes), jnp.float32)
    for s in range(0, sources, 2):
        code = jnp.where(
            low_half,
            received[s, live:, :].astype(jnp.float32),
            received[s + 1, live:, :].astype(jnp.float32),
        )
        one_hot = jnp.concatenate(
            [jnp.where(code == r, jnp.float32(1.0), jnp.float32(0.0)) for r in row_ids], axis=0
        ).astype(jnp.bfloat16)
        block = received[s : s + 2, :live, :].reshape(2 * live, lanes)
        total = total + jnp.dot(one_hot, block, preferred_element_type=jnp.float32)
    summed[...] = total
    squares[...] = jnp.sum((total * total).reshape(total_rows // BLK, BLK, lanes), axis=0)


def deposit(received, row_count):
    lanes = received.shape[2]
    return pl.pallas_call(
        deposit_kernel,
        out_shape=(
            jax.ShapeDtypeStruct((row_count, lanes), jnp.float32),
            jax.ShapeDtypeStruct((BLK, lanes), jnp.float32),
        ),
        in_specs=[pl.BlockSpec(memory_space=pltpu.VMEM)],
        out_specs=(pl.BlockSpec(memory_space=pltpu.VMEM), pl.BlockSpec(memory_space=pltpu.VMEM)),
        name="deposit",
    )(received)


def per_device(gradient, residual, block_ids, block_counts):
    row_count, width = gradient.shape
    replicas = lax.axis_size(REPLICA)
    block_total = row_count // BLK
    packed = pack(gradient, residual, block_ids, block_counts, replicas)
    received = lax.all_to_all(packed, REPLICA, split_axis=0, concat_axis=0, tiled=True)

    slot_ids = block_ids[0]
    live_slot = jnp.arange(slot_ids.shape[0], dtype=jnp.int32) < block_counts[0, 0]
    hit_table = (
        slot_ids[:, None] == jnp.arange(block_total, dtype=jnp.int32)[None, :]
    ) & live_slot[:, None]
    row_chosen = jnp.repeat(jnp.any(hit_table, axis=0), BLK)[:, None]
    accumulated = gradient.astype(jnp.float32) + residual
    sent = jnp.where(
        row_chosen, accumulated.astype(jnp.bfloat16).astype(jnp.float32), jnp.float32(0.0)
    )
    new_residual = accumulated - sent

    summed, squares = deposit(received, row_count)
    squares = squares.sum(axis=0, keepdims=True)
    squares = squares + lax.ppermute(squares, "section_1", [(0, 1), (1, 0)])
    chips = lax.axis_size(CHIPS)
    copies = jnp.broadcast_to(squares[None], (chips, *squares.shape))
    everyone = lax.all_to_all(copies, CHIPS, split_axis=0, concat_axis=0, tiled=True)
    norm_total = jnp.sum(everyone)
    element_count = lax.axis_size(SECTION) * row_count * width
    root_mean = jnp.sqrt(norm_total / element_count + epsilon)
    clip_factor = scale_level / root_mean
    update = (summed * clip_factor).astype(jnp.bfloat16)
    return (new_residual, update)


def solution(mesh):
    split = Mesh(
        mesh.devices.reshape(4, 2, 8, 4), ("section_0", "section_1", "replica_0", "replica_1")
    )
    return jax.shard_map(
        per_device,
        mesh=split,
        in_specs=(
            P(SECTION, REPLICA),
            P(SECTION, REPLICA),
            P(SECTION, REPLICA),
            P(SECTION, REPLICA),
        ),
        out_specs=(P(SECTION, REPLICA), P(SECTION, REPLICA)),
        check_vma=False,
    )
```
